128 devices in a mesh: frames: 32 (over x, z, core), heads: 4 (over y).
Axes of the slice: x: 4, y: 4, z: 4, core: 2. Of those that a mesh axis runs over, the one named last changes fastest.
Arguments:
- queries: bfloat16 [32768, 2560], P('frames', 'heads'), may hold values from -6 to 6, as said below
- keys: bfloat16 [32768, 2560], P('frames', 'heads'), may hold values from -6 to 6, as said below
- values: bfloat16 [32768, 2560], P('frames', 'heads'), may hold values from -6 to 6
- block_ids: int32 [256, 4], replicated, may hold values from 0 to 255, as said below
- counts: int32 [256], P('frames'), may hold values from 1 to 4
- w_out: bfloat16 [2560, 5120], P('heads'), may hold values from -0.125 to 0.125
Outputs:
- projected: bfloat16 [32768, 5120], P('frames', 'heads')
The draws below stay inside these ranges and needn't reach their ends.
Inputs may be any that keep to these rules, and one draw needn't show every extreme that they name: `block_ids`: block j is held by index j // 8 of frames. Counted with repeats, the entries of the 8 query blocks of one index of frames name at most 2 blocks held by any one index, and exactly 2 held by some index. Entries of a row may repeat. `queries`: drawn in float32 and rounded once. `keys`: drawn in float32 and rounded once.
All inputs are finite; a program needn't handle non-finite values.
Results may differ from the reference program's by a relative error of at most 0.0052.
Values may be sent and summed in bfloat16 or wider, within the bound.
A program may use at most 192 MiB of HBM per device.

```python
import jax
import jax.numpy as jnp
from jax import lax

D = 5120
HEADS = 20
DH = 128
TILE = 128
SEL = 4
BLK_DEV = 8
NB = 256
TOKENS = 32768
CAP = 2
N_FRAMES = 32


def pair_draw(key, which_one):
    base = jax.random.fold_in(key, 7)
    key_query, key_key = jax.random.split(base, 2)
    full_shape = (TOKENS, HEADS * DH)
    query_part = jnp.clip(1.5 * jax.random.normal(key_query, full_shape, jnp.float32), -6.0, 6.0)
    key_part = jnp.clip(1.5 * jax.random.normal(key_key, full_shape, jnp.float32), -6.0, 6.0)
    if which_one == 0:
        return query_part
    return key_part


def draw_queries(key, part):
    return pair_draw(key, 0).astype(jnp.bfloat16)


def draw_keys(key, part):
    return pair_draw(key, 1).astype(jnp.bfloat16)


def draw_block_ids(key, part):
    requests = BLK_DEV * SEL

    def one_device(device_key):
        key_star, key_order, key_shuffle, key_local = jax.random.split(device_key, 4)
        owners = jnp.tile(jnp.arange(N_FRAMES, dtype=jnp.int32), CAP)
        star = jax.random.randint(key_star, (), 0, N_FRAMES, dtype=jnp.int32)
        order = jax.random.permutation(key_order, N_FRAMES * CAP).astype(jnp.int32)
        priority = order + jnp.where(owners == star, 0, N_FRAMES * CAP).astype(jnp.int32)
        picked = owners[jnp.argsort(priority, stable=True)][:requests]
        shuffled = picked[jax.random.permutation(key_shuffle, requests)]
        local_block = jax.random.randint(key_local, (requests,), 0, BLK_DEV, dtype=jnp.int32)
        return shuffled * BLK_DEV + local_block
    device_keys = jax.vmap(lambda device: jax.random.fold_in(key, 100 + device))(jnp.arange(N_FRAMES))
    return jax.vmap(one_device)(device_keys).reshape(NB, SEL).astype(jnp.int32)


def place_ends(array, key, least, top_value):
    spot = [jax.random.randint(jax.random.fold_in(key, axis), (), 0, length) for axis, length in enumerate(array.shape)]
    main_axis = array.shape.index(max(array.shape))
    beside = spot[:main_axis] + [(spot[main_axis] + 1) % array.shape[main_axis]] + spot[main_axis + 1:]
    return array.at[tuple(spot)].set(least).at[tuple(beside)].set(top_value)


def level_of(own_key, shape, cuts, least, top_value):
    def one(axis_at, shards_of):
        draws = jax.random.uniform(jax.random.fold_in(jax.random.fold_in(own_key, 6), axis_at), (shards_of,), jnp.float32, least / len(cuts), top_value / len(cuts))
        return jnp.repeat(jnp.exp(draws), shape[axis_at] // shards_of).reshape((-1,) + (1,) * (len(shape) - axis_at - 1))

    loudness = one(*cuts[0])
    for cut in cuts[1:]:
        loudness = loudness * one(*cut)
    return loudness


def normal_values(key, extent, scale, reach, cuts=(), kind=jnp.bfloat16):
    loudness = level_of(key, extent, cuts, -0.22, 0.18) if cuts else 1.0
    array = jax.random.normal(key, extent, jnp.float32) * scale * loudness
    return jnp.minimum(jnp.maximum(array, -reach), reach).astype(kind)


def setup_inputs(seed: int = 0) -> dict:
    arg_keys = jax.random.split(jax.random.key(seed), 7)
    queries = draw_queries(jax.random.fold_in(arg_keys[6], 71), 0)
    keys = draw_keys(jax.random.fold_in(arg_keys[6], 71), 0)
    values = normal_values(arg_keys[2], (TOKENS, HEADS * DH), 1.0, 6.0, ((0, 32), (1, 4)))
    block_ids = draw_block_ids(jax.random.fold_in(arg_keys[6], 71), 0)
    counts = place_ends(jax.random.randint(arg_keys[4], (NB,), 1, SEL + 1), jax.random.fold_in(arg_keys[4], 1), 1, SEL).astype(jnp.int32)
    w_out = normal_values(arg_keys[5], (HEADS * DH, D), (HEADS * DH) ** -0.5, 0.125, ((0, 4),))
    return {"queries": queries, "keys": keys, "values": values, "block_ids": block_ids, "counts": counts, "w_out": w_out}


def reference(queries, keys, values, block_ids, counts, w_out):
    full_width = HEADS * DH
    inv_root = 1.0 / (DH ** 0.5)
    query_tiles = queries.reshape(NB, TILE, full_width)
    key_tiles = keys.reshape(NB, TILE, full_width)
    value_tiles = values.reshape(NB, TILE, full_width)

    def one_block(block_index):
        chosen = block_ids[block_index]
        keyset_k = jnp.concatenate([key_tiles[block_index][None], key_tiles[chosen]], 0)
        keyset_v = jnp.concatenate([value_tiles[block_index][None], value_tiles[chosen]], 0)
        keyset_k = keyset_k.reshape((SEL + 1) * TILE, HEADS, DH).astype(jnp.float32)
        keyset_v = keyset_v.reshape((SEL + 1) * TILE, HEADS, DH).astype(jnp.float32)
        query_tile = query_tiles[block_index].reshape(TILE, HEADS, DH).astype(jnp.float32)
        scores = jnp.einsum("qhd,khd->hqk", query_tile, keyset_k) * inv_root
        allowed = jnp.concatenate([jnp.ones((1,), bool), jnp.arange(SEL) < counts[block_index]])
        key_allowed = jnp.repeat(allowed, TILE)
        scores = jnp.where(key_allowed[None, None, :], scores, -jnp.inf)
        row_max = jnp.max(scores, axis=-1, keepdims=True)
        probs = jnp.exp(scores - row_max)
        denom_sum = jnp.sum(probs, axis=-1)
        weights = lax.optimization_barrier(probs.astype(jnp.bfloat16)).astype(jnp.float32)
        mixed = jnp.einsum("hqk,khd->qhd", weights, keyset_v)
        mixed = mixed / jnp.transpose(denom_sum)[:, :, None]
        return mixed.astype(jnp.bfloat16).reshape(TILE, full_width)

    attn = lax.map(one_block, jnp.arange(NB)).reshape(TOKENS, full_width)
    return jnp.dot(attn, w_out, preferred_element_type=jnp.float32).astype(jnp.bfloat16)
```

```python
import math

import jax
import jax.numpy as jnp
from jax import lax
from jax.experimental import pallas as pl
from jax.experimental.pallas import tpu as pltpu
from jax.sharding import PartitionSpec as P

DH = 128
TILE = 128
SEL = 4
RING = 4
HEADS_HERE = 5
BLOCKS = 8
TOK = BLOCKS * TILE
HALF = TOK // 2
WIDTH = HEADS_HERE * DH
FEAT = 1280
NEG = -1e30
TO_LOG2 = math.log2(math.e) / math.sqrt(DH)


def all_waited(copies):
    for copy in copies:
        copy.wait_send()


def kernel(
    ids, cnt, q_in, k_in, v_in, w_in, out,
    QB, CB, OB, OWN, RLY, OIN, LB, LRLY, LIN, AT, W, ACC,
    send_sem, recv_sem, local_sem, *kv_bufs,
):
    KB, VB = kv_bufs[:HEADS_HERE], kv_bufs[HEADS_HERE:]
    f = lax.axis_index("frames")
    py = lax.axis_index("heads")
    px = f // 8
    pz = (f // 2) % 4
    c = f % 2

    def frame(x, z, core):
        return (x * 4 + z) * 2 + core

    def up(p):
        return (p + 1) % 4

    def down(p):
        return (p + 3) % 4

    x_right, x_left = (frame(up(px), pz, c), py), (frame(down(px), pz, c), py)
    z_right, z_left = (frame(px, up(pz), c), py), (frame(px, down(pz), c), py)
    z_far = (frame(px, (pz + 2) % 4, c), py)
    y_right, y_left, y_far = (f, up(py)), (f, down(py)), (f, (py + 2) % 4)
    sibling = (frame(px, pz, 1 - c), py)
    partners = [x_right, x_left, z_right, z_left, z_far, y_right, y_left, y_far, sibling]

    barrier = pltpu.get_barrier_semaphore()
    for device in partners:
        pl.semaphore_signal(barrier, inc=1, device_id=device, device_id_type=MESH)
    pl.semaphore_wait(barrier, len(partners))

    used = [0]
    used_local = [0]
    sent = []

    def remote(src, dst, device):
        i = used[0]
        used[0] += 1
        return pltpu.make_async_remote_copy(
            src_ref=src, dst_ref=dst, send_sem=send_sem.at[i], recv_sem=recv_sem.at[i],
            device_id=device, device_id_type=MESH,
        )

    def local(src, dst):
        i = used_local[0]
        used_local[0] += 1
        return pltpu.make_async_copy(src, dst, local_sem.at[i])

    def go(copies):
        for copy in copies:
            copy.start()
            sent.append(copy)

    def cols(h):
        return pl.ds(h * DH, DH)

    heads = range(HEADS_HERE)
    lo, hi = pl.ds(0, HALF), pl.ds(HALF, HALF)

    def slot(s, part=None):
        if part is None:
            return pl.ds(s * BLOCKS, BLOCKS)
        return pl.ds(s * BLOCKS + part * (BLOCKS // 2), BLOCKS // 2)

    kv = []
    for h in heads:
        hc = cols(h)
        first, fwd, sib_own, sib_near, sib_far, own = [], [], [], [], [], []
        for src, buf in ((k_in, KB[h]), (v_in, VB[h])):
            mine = src.at[:, :, hc]
            first.append((remote(mine, buf.at[slot(2)], x_right),
                          remote(mine, buf.at[slot(6)], x_left)))
            fwd.append((remote(buf.at[slot(2, 0)], buf.at[slot(4, 0)], x_right),
                        remote(buf.at[slot(6, 1)], buf.at[slot(4, 1)], x_left)))
            sib_own.append(remote(mine, buf.at[slot(1)], sibling))
            sib_near.append((remote(buf.at[slot(2)], buf.at[slot(3)], sibling),
                             remote(buf.at[slot(6)], buf.at[slot(7)], sibling)))
            sib_far.append((remote(buf.at[slot(4, 0)], buf.at[slot(5, 0)], sibling),
                            remote(buf.at[slot(4, 1)], buf.at[slot(5, 1)], sibling)))
            own.append(local(mine, buf.at[slot(0)]))
        kv.append((first, fwd, sib_own, sib_near, sib_far, own))

    def ring(src, dst_near, dst_far, device_right, device_left, hc):
        first = (remote(src, dst_near[0].at[:, hc], device_right),
                 remote(src, dst_near[1].at[:, hc], device_left))
        fwd = (remote(dst_near[0].at[lo, hc], dst_far.at[lo, hc], device_right),
               remote(dst_near[1].at[hi, hc], dst_far.at[hi, hc], device_left))
        return first, fwd

    qs = []
    for h in heads:
        mine = q_in.at[:, cols(h)]
        first, fwd = ring(mine, (QB.at[1], QB.at[3]), QB.at[2], z_right, z_left, cols(h))
        qs.append((first, fwd, local(mine, QB.at[0, :, cols(h)])))
    ys = [ring(AT.at[0, :, cols(h)], (AT.at[1], AT.at[3]), AT.at[2], y_right, y_left, cols(h))
          for h in heads]

    os = []
    for h in heads:
        hc = cols(h)
        relay = (remote(OB.at[2, lo, hc], RLY.at[0, :, hc], z_right),
                 remote(LB.at[2, h, pl.ds(0, 4)], LRLY.at[0, h], z_right),
                 remote(OB.at[2, hi, hc], RLY.at[1, :, hc], z_left),
                 remote(LB.at[2, h, pl.ds(4, 4)], LRLY.at[1, h], z_left))
        back = (remote(OB.at[3, :, hc], OIN.at[0, :, hc], z_right),
                remote(LB.at[3, h], LIN.at[0, h], z_right),
                remote(OB.at[1, :, hc], OIN.at[1, :, hc], z_left),
                remote(LB.at[1, h], LIN.at[1, h], z_left))
        os.append((relay, back))

    rows_w = pl.ds(pl.multiple_of(c * (WIDTH // 2), WIDTH // 2), WIDTH // 2)

    def w_cols(y):
        return pl.ds(pl.multiple_of(y * FEAT, FEAT), FEAT)

    w_first = [remote(w_in.at[rows_w, w_cols(dev[1])], W.at[s, rows_w, :], dev)
               for s, dev in ((1, y_right), (3, y_left), (2, y_far))]
    w_sib = [remote(W.at[s, rows_w, :], W.at[s, rows_w, :], sibling) for s in (1, 3, 2)]
    w_own = local(w_in.at[:, w_cols(py)], W.at[0])
    cnt_copies = [remote(cnt, CB.at[s], dev) for s, dev in ((1, z_right), (3, z_left), (2, z_far))]

    def issue(h):
        first, _, sib_own, _, _, own = kv[h]
        go(qs[h][0])
        for pair in first:
            go(pair)
        go(sib_own)
        for copy in own + [qs[h][2]]:
            copy.start()

    def forward(h):
        first, fwd, _, sib_near, _, _ = kv[h]
        for t in range(2):
            for side in range(2):
                first[t][side].wait_recv()
                go([fwd[t][side], sib_near[t][side]])
        for side in range(2):
            qs[h][0][side].wait_recv()
            go([qs[h][1][side]])

    def ready(h):
        _, fwd, sib_own, sib_near, sib_far, own = kv[h]
        for t in range(2):
            for side in range(2):
                fwd[t][side].wait_recv()
                go([sib_far[t][side]])
        for side in range(2):
            qs[h][1][side].wait_recv()
        for copy in own + [qs[h][2]]:
            copy.wait()
        for t in range(2):
            sib_own[t].wait_recv()
            for side in range(2):
                sib_near[t][side].wait_recv()
            for side in range(2):
                sib_far[t][side].wait_recv()

    eye = lax.broadcasted_iota(jnp.int32, (TILE, TILE), 0) == lax.broadcasted_iota(
        jnp.int32, (TILE, TILE), 1)

    def as_row(col):
        return jnp.sum(jnp.where(eye, col, 0.0), axis=0, keepdims=True)

    def as_col(row):
        return jnp.sum(jnp.where(eye, row, 0.0), axis=1, keepdims=True)

    def attend(r, h, j):
        hc = cols(h)
        q = QB[r, pl.ds(pl.multiple_of(j * TILE, TILE), TILE), hc]
        q_block = frame(px, (pz + 4 - r) % 4, c) * BLOCKS + j
        limit = CB[r, pl.ds(j, 1), :]
        scores, vals = [], []
        for s in range(SEL):
            block = ids[q_block * SEL + s]
            xs, zs, cs = block >> 6, (block >> 4) & 3, (block >> 3) & 1
            place = ((((px + 4 - xs) & 3) * 2 + ((cs + c) & 1)) * BLOCKS) + (block & 7)
            here = jnp.where(zs == pz, 0.0, NEG)
            bias = jnp.where(limit > s, here, NEG)
            k = KB[h][place]
            vals.append(VB[h][place])
            scores.append(lax.dot_general(q, k, (((1,), (1,)), ((), ())),
                                          preferred_element_type=jnp.float32) * TO_LOG2 + bias)
        if r == 0:
            vals.append(VB[h][j])
            scores.append(lax.dot_general(q, KB[h][j], (((1,), (1,)), ((), ())),
                                          preferred_element_type=jnp.float32) * TO_LOG2)
        top = scores[0]
        for t in scores[1:]:
            top = jnp.maximum(top, t)
        top = jnp.max(top, axis=1, keepdims=True)
        probs = [jnp.exp2(t - top) for t in scores]
        total = probs[0]
        for p in probs[1:]:
            total = total + p
        total = jnp.sum(total, axis=1, keepdims=True)
        o = jnp.dot(jnp.concatenate([p.astype(jnp.bfloat16) for p in probs], axis=1),
                    jnp.concatenate(vals, axis=0), preferred_element_type=jnp.float32)
        return o * (1.0 / total), top + jnp.log2(total)

    def merge(parts):
        top = parts[0][1]
        for _, l in parts[1:]:
            top = jnp.maximum(top, l)
        mass, o = 0.0, 0.0
        for po, l in parts:
            a = jnp.exp2(l - top)
            mass = mass + a
            o = o + po.astype(jnp.float32) * a
        return o * (1.0 / mass), top + jnp.log2(mass)

    def over(first_block, n, body):
        def pair(i, carry):
            for u in range(2):
                body(first_block + i * 2 + u)
            return carry
        lax.fori_loop(0, n // 2, pair, 0)

    def block_rows(j):
        return pl.ds(pl.multiple_of(j * TILE, TILE), TILE)

    def plain(r, h):
        def body(j):
            o, l = attend(r, h, j)
            OB[r, block_rows(j), cols(h)] = o.astype(jnp.bfloat16)
            LB[r, h, j] = as_row(l)
        return body

    def merged(r, h, side, first_block):
        def body(j):
            o, l = attend(r, h, j)
            o, l = merge([(o, l), (RLY[side, block_rows(j - first_block), cols(h)],
                                   as_col(LRLY[side, h, j - first_block]))])
            OB[r, block_rows(j), cols(h)] = o.astype(jnp.bfloat16)
            LB[r, h, j] = as_row(l)
        return body

    def own_part(h):
        def body(j):
            o, l = attend(0, h, j)
            OWN[block_rows(j), cols(h)] = o
            LB[0, h, j] = as_row(l)
        return body

    def final(h):
        def body(j):
            parts = [(OWN[block_rows(j), cols(h)], as_col(LB[0, h, j]))]
            for side in range(2):
                parts.append((OIN[side, block_rows(j), cols(h)], as_col(LIN[side, h, j])))
            o, _ = merge(parts)
            AT[0, block_rows(j), cols(h)] = o.astype(jnp.bfloat16)
        return body

    def y_forward(h):
        first, fwd = ys[h]
        for side in range(2):
            first[side].wait_recv()
            go([fwd[side]])

    def project(h):
        for side in range(2):
            ys[h][1][side].wait_recv()
        last = h == HEADS_HERE - 1
        tile_n, tile_m = 256, 256

        def one(i, carry):
            cs = pl.ds(pl.multiple_of(i * tile_n, tile_n), tile_n)
            rhs = jnp.concatenate([W[r, pl.ds(h * DH, DH), cs] for r in range(RING)], axis=0)
            for m in range(TOK // tile_m):
                rs = pl.ds(m * tile_m, tile_m)
                lhs = jnp.concatenate([AT[r, rs, cols(h)] for r in range(RING)], axis=1)
                term = jnp.dot(lhs, rhs, preferred_element_type=jnp.float32)
                if h > 0:
                    term = term + ACC[rs, cs]
                if last:
                    out[rs, cs] = term.astype(jnp.bfloat16)
                else:
                    ACC[rs, cs] = term
            return carry

        lax.fori_loop(0, FEAT // tile_n, one, 0)

    CB[0] = cnt[...]
    go(cnt_copies)
    issue(0)
    issue(1)
    go(w_first)
    w_own.start()
    for copy in cnt_copies:
        copy.wait_recv()
    forward(0)
    issue(2)
    for h in heads:
        ready(h)
        if h + 1 < HEADS_HERE:
            forward(h + 1)
        if h + 3 < HEADS_HERE:
            issue(h + 3)
        over(0, 8, plain(2, h))
        go(os[h][0])
        if h == 1:
            for a, b in zip(w_first, w_sib):
                a.wait_recv()
                go([b])
        if h > 0:
            y_forward(h - 1)
        over(0, 8, own_part(h))
        over(4, 4, plain(3, h))
        over(0, 4, plain(1, h))
        for copy in os[h][0]:
            copy.wait_recv()
        over(0, 4, merged(3, h, 0, 0))
        over(4, 4, merged(1, h, 1, 4))
        go(os[h][1])
        if h == 1:
            for copy in w_sib:
                copy.wait_recv()
            w_own.wait()
        if h > 0:
            project(h - 1)
        for copy in os[h][1]:
            copy.wait_recv()
        over(0, 8, final(h))
        go(ys[h][0])
    y_forward(HEADS_HERE - 1)
    project(HEADS_HERE - 1)
    all_waited(sent)


MESH = pl.DeviceIdType.MESH
N_REMOTE = 5 * (18 + 4 + 4 + 8) + 6 + 3
N_LOCAL = 5 * 3 + 1


def shards(queries, keys, values, block_ids, counts, w_out):
    ids = block_ids.reshape(-1)
    cnt = jnp.broadcast_to(counts[:, None], (BLOCKS, 128))
    vmem = pl.BlockSpec(memory_space=pltpu.VMEM)
    hbm = pl.BlockSpec(memory_space=pl.ANY)
    bf16, f32 = jnp.bfloat16, jnp.float32
    return pl.pallas_call(
        kernel,
        out_shape=jax.ShapeDtypeStruct((TOK, FEAT), bf16),
        in_specs=[pl.BlockSpec(memory_space=pltpu.SMEM), vmem, hbm, hbm, hbm, hbm],
        out_specs=vmem,
        scratch_shapes=[
            pltpu.VMEM((4, TOK, WIDTH), bf16),
            pltpu.VMEM((4, BLOCKS, 128), jnp.int32),
            pltpu.VMEM((4, TOK, WIDTH), bf16),
            pltpu.VMEM((TOK, WIDTH), f32),
            pltpu.VMEM((2, HALF, WIDTH), bf16),
            pltpu.VMEM((2, TOK, WIDTH), bf16),
            pltpu.VMEM((4, HEADS_HERE, BLOCKS, 1, 128), f32),
            pltpu.VMEM((2, HEADS_HERE, BLOCKS // 2, 1, 128), f32),
            pltpu.VMEM((2, HEADS_HERE, BLOCKS, 1, 128), f32),
            pltpu.VMEM((4, TOK, WIDTH), bf16),
            pltpu.VMEM((4, WIDTH, FEAT), bf16),
            pltpu.VMEM((TOK, FEAT), f32),
            pltpu.SemaphoreType.DMA((N_REMOTE,)),
            pltpu.SemaphoreType.DMA((N_REMOTE,)),
            pltpu.SemaphoreType.DMA((N_LOCAL,)),
        ] + [pltpu.VMEM((8 * BLOCKS, TILE, DH), bf16)] * (2 * HEADS_HERE),
        compiler_params=pltpu.CompilerParams(
            collective_id=0, has_side_effects=True, vmem_limit_bytes=67043328),
        name="sparse_attention",
    )(ids, cnt, queries, keys.reshape(BLOCKS, TILE, WIDTH), values.reshape(BLOCKS, TILE, WIDTH), w_out)


def solution(mesh):
    placed = (
        P("frames", "heads"),
        P("frames", "heads"),
        P("frames", "heads"),
        P(),
        P("frames"),
        P("heads", None),
    )
    return jax.shard_map(
        shards, mesh=mesh, in_specs=placed, out_specs=P("frames", "heads"), check_vma=False
    )
```

```python
import math

import jax
import jax.numpy as jnp
from jax import lax
from jax.experimental import pallas as pl
from jax.experimental.pallas import tpu as pltpu
from jax.sharding import PartitionSpec as P

DH = 128
TILE = 128
SEL = 4
RING = 4
HEADS_HERE = 5
BLOCKS = 8
TOK = BLOCKS * TILE
HALF = TOK // 2
WIDTH = HEADS_HERE * DH
FEAT = 1280
NEG = -1e30
TO_LOG2 = math.log2(math.e) / math.sqrt(DH)


def all_waited(copies):
    for copy in copies:
        copy.wait_send()


def kernel(
    ids, cnt, q_in, k_in, v_in, w_in, out,
    QB, CB, VIN, OB, OWN, RLY, OIN, LB, LRLY, LIN, AT, W, ACC,
    send_sem, recv_sem, local_sem, *kv_bufs,
):
    KB, VB = kv_bufs[:HEADS_HERE], kv_bufs[HEADS_HERE:]
    f = lax.axis_index("frames")
    py = lax.axis_index("heads")
    px = f // 8
    pz = (f // 2) % 4
    c = f % 2

    def frame(x, z, core):
        return (x * 4 + z) * 2 + core

    def up(p):
        return (p + 1) % 4

    def down(p):
        return (p + 3) % 4

    x_right, x_left = (frame(up(px), pz, c), py), (frame(down(px), pz, c), py)
    z_right, z_left = (frame(px, up(pz), c), py), (frame(px, down(pz), c), py)
    z_far = (frame(px, (pz + 2) % 4, c), py)
    y_right, y_left, y_far = (f, up(py)), (f, down(py)), (f, (py + 2) % 4)
    sibling = (frame(px, pz, 1 - c), py)
    partners = [x_right, x_left, z_right, z_left, z_far, y_right, y_left, y_far, sibling]

    barrier = pltpu.get_barrier_semaphore()
    for device in partners:
        pl.semaphore_signal(barrier, inc=1, device_id=device, device_id_type=MESH)
    pl.semaphore_wait(barrier, len(partners))

    used = [0]
    used_local = [0]
    sent = []

    def remote(src, dst, device):
        i = used[0]
        used[0] += 1
        return pltpu.make_async_remote_copy(
            src_ref=src, dst_ref=dst, send_sem=send_sem.at[i], recv_sem=recv_sem.at[i],
            device_id=device, device_id_type=MESH,
        )

    def local(src, dst):
        i = used_local[0]
        used_local[0] += 1
        return pltpu.make_async_copy(src, dst, local_sem.at[i])

    def go(copies):
        for copy in copies:
            copy.start()
            sent.append(copy)

    def cols(h):
        return pl.ds(h * DH, DH)

    heads = range(HEADS_HERE)
    lo, hi = pl.ds(0, HALF), pl.ds(HALF, HALF)

    def slot(s, part=None):
        if part is None:
            return pl.ds(s * BLOCKS, BLOCKS)
        return pl.ds(s * BLOCKS + part * (BLOCKS // 2), BLOCKS // 2)

    kv = []
    for h in heads:
        hc = cols(h)
        first, fwd, sib_own, sib_near, sib_far, own = [], [], [], [], [], []
        for mine, buf in ((k_in.at[:, :, hc], KB[h]), (VB[h].at[slot(0)], VB[h])):
            first.append((remote(mine, buf.at[slot(2)], x_right),
                          remote(mine, buf.at[slot(6)], x_left)))
            fwd.append((remote(buf.at[slot(2, 0)], buf.at[slot(4, 0)], x_right),
                        remote(buf.at[slot(6, 1)], buf.at[slot(4, 1)], x_left)))
            sib_own.append(remote(mine, buf.at[slot(1)], sibling))
            sib_near.append((remote(buf.at[slot(2)], buf.at[slot(3)], sibling),
                             remote(buf.at[slot(6)], buf.at[slot(7)], sibling)))
            sib_far.append((remote(buf.at[slot(4, 0)], buf.at[slot(5, 0)], sibling),
                            remote(buf.at[slot(4, 1)], buf.at[slot(5, 1)], sibling)))
        own.append(local(k_in.at[:, :, hc], KB[h].at[slot(0)]))
        kv.append((first, fwd, sib_own, sib_near, sib_far, own))

    def ring(src, buf, h, device_right, device_left):
        first = (remote(src, buf.at[1, h], device_right), remote(src, buf.at[3, h], device_left))
        fwd = (remote(buf.at[1, h, lo], buf.at[2, h, lo], device_right),
               remote(buf.at[3, h, hi], buf.at[2, h, hi], device_left))
        return first, fwd

    qs = []
    for h in heads:
        mine = q_in.at[:, cols(h)]
        first, fwd = ring(mine, QB, h, z_right, z_left)
        qs.append((first, fwd, local(mine, QB.at[0, h])))
    ys = [ring(AT.at[0, h], AT, h, y_right, y_left) for h in heads]

    os = []
    for h in heads:
        first4, last4 = pl.ds(0, BLOCKS // 2), pl.ds(BLOCKS // 2, BLOCKS // 2)
        relay = (remote(OB.at[2, h, first4], RLY.at[0, h], z_right),
                 remote(LB.at[2, h, first4], LRLY.at[0, h], z_right),
                 remote(OB.at[2, h, last4], RLY.at[1, h], z_left),
                 remote(LB.at[2, h, last4], LRLY.at[1, h], z_left))
        back = (remote(OB.at[3, h], OIN.at[0, h], z_right),
                remote(LB.at[3, h], LIN.at[0, h], z_right),
                remote(OB.at[1, h], OIN.at[1, h], z_left),
                remote(LB.at[1, h], LIN.at[1, h], z_left))
        os.append((relay, back))

    rows_w = pl.ds(pl.multiple_of(c * (WIDTH // 2), WIDTH // 2), WIDTH // 2)

    def w_cols(y):
        return pl.ds(pl.multiple_of(y * FEAT, FEAT), FEAT)

    w_first = [remote(w_in.at[rows_w, w_cols(dev[1])], W.at[s, rows_w, :], dev)
               for s, dev in ((1, y_right), (3, y_left), (2, y_far))]
    w_sib = [remote(W.at[s, rows_w, :], W.at[s, rows_w, :], sibling) for s in (1, 3, 2)]
    w_own = local(w_in.at[:, w_cols(py)], W.at[0])
    cnt_copies = [remote(CB.at[0], CB.at[s], dev) for s, dev in ((1, z_right), (3, z_left), (2, z_far))]

    def flip_values(h):
        def one(j, carry):
            VB[h][j] = VIN[j, :, cols(h)].T
            return carry
        lax.fori_loop(0, BLOCKS, one, 0)

    def issue(h):
        first, _, sib_own, _, _, own = kv[h]
        go(first[0])
        go(qs[h][0])
        go([sib_own[0]])
        for copy in own + [qs[h][2]]:
            copy.start()
        flip_values(h)
        go(first[1])
        go([sib_own[1]])

    def forward(h):
        first, fwd, _, sib_near, _, _ = kv[h]
        for t in range(2):
            for side in range(2):
                first[t][side].wait_recv()
                go([fwd[t][side], sib_near[t][side]])
        for side in range(2):
            qs[h][0][side].wait_recv()
            go([qs[h][1][side]])

    def ready(h):
        _, fwd, sib_own, sib_near, sib_far, own = kv[h]
        for t in range(2):
            for side in range(2):
                fwd[t][side].wait_recv()
                go([sib_far[t][side]])
        for side in range(2):
            qs[h][1][side].wait_recv()
        for copy in own + [qs[h][2]]:
            copy.wait()
        for t in range(2):
            sib_own[t].wait_recv()
            for side in range(2):
                sib_near[t][side].wait_recv()
            for side in range(2):
                sib_far[t][side].wait_recv()

    def attend(r, h, j):
        q = QB[r, h, block_rows(j)]
        q_block = frame(px, (pz + 4 - r) % 4, c) * BLOCKS + j
        limit = CB[r, pl.ds(j, 1), :]
        scores, biases, vals = [], [], []
        for s in range(SEL):
            block = ids[s, q_block]
            xs, zs, cs = block >> 6, (block >> 4) & 3, (block >> 3) & 1
            place = ((((px + 4 - xs) & 3) * 2 + ((cs + c) & 1)) * BLOCKS) + (block & 7)
            here = jnp.where(zs == pz, 0.0, NEG)
            biases.append(jnp.where(limit > s, here, NEG))
            vals.append(VB[h][place])
            scores.append(lax.dot_general(KB[h][place], q, (((1,), (1,)), ((), ())),
                                          preferred_element_type=jnp.float32))
        if r == 0:
            biases.append(jnp.zeros((1, TILE), jnp.float32))
            vals.append(VB[h][j])
            scores.append(lax.dot_general(KB[h][j], q, (((1,), (1,)), ((), ())),
                                          preferred_element_type=jnp.float32))
        top = jnp.full((1, TILE), NEG * 0.1, jnp.float32)
        for t, b in zip(scores, biases):
            top = jnp.maximum(top, jnp.max(t, axis=0, keepdims=True) * TO_LOG2 + b)
        probs = [jnp.exp2(t * TO_LOG2 + (b - top)) for t, b in zip(scores, biases)]
        total = probs[0]
        for p in probs[1:]:
            total = total + p
        total = jnp.maximum(jnp.sum(total, axis=0, keepdims=True), 1e-30)
        o = jnp.dot(jnp.concatenate(vals, axis=1),
                    jnp.concatenate([p.astype(jnp.bfloat16) for p in probs], axis=0),
                    preferred_element_type=jnp.float32)
        return o * (1.0 / total), top + jnp.log2(total)

    def merge(parts):
        top = parts[0][1]
        for _, l in parts[1:]:
            top = jnp.maximum(top, l)
        ws = [jnp.exp2(l - top) for _, l in parts]
        mass = ws[0]
        for a in ws[1:]:
            mass = mass + a
        inv = 1.0 / mass
        o = 0.0
        for (po, _), a in zip(parts, ws):
            o = o + po.astype(jnp.float32) * (a * inv)
        return o, top + jnp.log2(mass)

    def over(first_block, n, body):
        def pair(i, carry):
            for u in range(2):
                body(first_block + i * 2 + u)
            return carry
        lax.fori_loop(0, n // 2, pair, 0)

    def block_rows(j):
        return pl.ds(pl.multiple_of(j * TILE, TILE), TILE)

    def plain(r, h):
        def body(j):
            o, l = attend(r, h, j)
            OB[r, h, j] = o.astype(jnp.bfloat16)
            LB[r, h, j] = l
        return body

    def merged(r, h, side, first_block):
        def body(j):
            o, l = merge([attend(r, h, j),
                          (RLY[side, h, j - first_block], LRLY[side, h, j - first_block])])
            OB[r, h, j] = o.astype(jnp.bfloat16)
            LB[r, h, j] = l
        return body

    def own_part(h):
        def body(j):
            o, l = attend(0, h, j)
            OWN[h, j] = o
            LB[0, h, j] = l
        return body

    def final(h):
        def body(j):
            parts = [(OWN[h, j], LB[0, h, j])]
            for side in range(2):
                parts.append((OIN[side, h, j], LIN[side, h, j]))
            o, _ = merge(parts)
            AT[0, h, block_rows(j)] = o.T.astype(jnp.bfloat16)
        return body

    def y_forward(h):
        first, fwd = ys[h]
        for side in range(2):
            first[side].wait_recv()
            go([fwd[side]])

    def project(h):
        for side in range(2):
            ys[h][1][side].wait_recv()
        last = h == HEADS_HERE - 1
        tile_n, tile_m = 256, 256

        def one(i, carry):
            cs = pl.ds(pl.multiple_of(i * tile_n, tile_n), tile_n)
            rhs = jnp.concatenate([W[r, pl.ds(h * DH, DH), cs] for r in range(RING)], axis=0)
            for m in range(TOK // tile_m):
                rs = pl.ds(m * tile_m, tile_m)
                lhs = jnp.concatenate([AT[r, h, rs] for r in range(RING)], axis=1)
                term = jnp.dot(lhs, rhs, preferred_element_type=jnp.float32)
                if h > 0:
                    term = term + ACC[rs, cs]
                if last:
                    out[rs, cs] = term.astype(jnp.bfloat16)
                else:
                    ACC[rs, cs] = term
            return carry

        lax.fori_loop(0, FEAT // tile_n, one, 0)

    values_in = local(v_in, VIN)
    values_in.start()
    for j in range(BLOCKS):
        CB[0, pl.ds(j, 1), :] = jnp.full((1, 128), cnt[j], jnp.int32)
    values_in.wait()
    issue(0)
    go(cnt_copies)
    issue(1)
    go(w_first)
    w_own.start()
    for copy in cnt_copies:
        copy.wait_recv()
    forward(0)
    issue(2)

    def finish(h):
        for copy in os[h][1]:
            copy.wait_recv()
        over(0, 8, final(h))
        go(ys[h][0])

    for h in heads:
        ready(h)
        if h + 1 < HEADS_HERE:
            forward(h + 1)
        if h + 3 < HEADS_HERE:
            issue(h + 3)
        over(0, 8, plain(2, h))
        go(os[h][0])
        if h == 1:
            for a, b in zip(w_first, w_sib):
                a.wait_recv()
                go([b])
        if h == 2:
            for copy in w_sib:
                copy.wait_recv()
            w_own.wait()
        if h > 0:
            finish(h - 1)
        if h > 1:
            project(h - 2)
        over(0, 8, own_part(h))
        over(4, 4, plain(3, h))
        over(0, 4, plain(1, h))
        for copy in os[h][0]:
            copy.wait_recv()
        over(0, 4, merged(3, h, 0, 0))
        over(4, 4, merged(1, h, 1, 4))
        go(os[h][1])
        if h > 0:
            y_forward(h - 1)
    finish(HEADS_HERE - 1)
    project(HEADS_HERE - 2)
    y_forward(HEADS_HERE - 1)
    project(HEADS_HERE - 1)
    all_waited(sent)


MESH = pl.DeviceIdType.MESH
N_REMOTE = 5 * (18 + 4 + 4 + 8) + 6 + 3
N_LOCAL = 5 * 2 + 2


def shards(queries, keys, values, block_ids, counts, w_out):
    smem = pl.BlockSpec(memory_space=pltpu.SMEM)
    vmem = pl.BlockSpec(memory_space=pltpu.VMEM)
    hbm = pl.BlockSpec(memory_space=pl.ANY)
    bf16, f32 = jnp.bfloat16, jnp.float32
    return pl.pallas_call(
        kernel,
        out_shape=jax.ShapeDtypeStruct((TOK, FEAT), bf16),
        in_specs=[smem, smem, hbm, hbm, hbm, hbm],
        out_specs=vmem,
        scratch_shapes=[
            pltpu.VMEM((4, HEADS_HERE, TOK, DH), bf16),
            pltpu.VMEM((4, BLOCKS, 128), jnp.int32),
            pltpu.VMEM((BLOCKS, TILE, WIDTH), bf16),
            pltpu.VMEM((4, HEADS_HERE, BLOCKS, DH, TILE), bf16),
            pltpu.VMEM((HEADS_HERE, BLOCKS, DH, TILE), f32),
            pltpu.VMEM((2, HEADS_HERE, BLOCKS // 2, DH, TILE), bf16),
            pltpu.VMEM((2, HEADS_HERE, BLOCKS, DH, TILE), bf16),
            pltpu.VMEM((4, HEADS_HERE, BLOCKS, 1, 128), f32),
            pltpu.VMEM((2, HEADS_HERE, BLOCKS // 2, 1, 128), f32),
            pltpu.VMEM((2, HEADS_HERE, BLOCKS, 1, 128), f32),
            pltpu.VMEM((4, HEADS_HERE, TOK, DH), bf16),
            pltpu.VMEM((4, WIDTH, FEAT), bf16),
            pltpu.VMEM((TOK, FEAT), f32),
            pltpu.SemaphoreType.DMA((N_REMOTE,)),
            pltpu.SemaphoreType.DMA((N_REMOTE,)),
            pltpu.SemaphoreType.DMA((N_LOCAL,)),
        ] + [pltpu.VMEM((8 * BLOCKS, TILE, DH), bf16)] * (2 * HEADS_HERE),
        compiler_params=pltpu.CompilerParams(
            collective_id=0, has_side_effects=True, vmem_limit_bytes=67043328),
        name="sparse_attention",
    )(block_ids.T, counts, queries, keys.reshape(BLOCKS, TILE, WIDTH), values.reshape(BLOCKS, TILE, WIDTH), w_out)


def solution(mesh):
    placed = (
        P("frames", "heads"),
        P("frames", "heads"),
        P("frames", "heads"),
        P(),
        P("frames"),
        P("heads", None),
    )
    return jax.shard_map(
        shards, mesh=mesh, in_specs=placed, out_specs=P("frames", "heads"), check_vma=False
    )
```

```python
import math

import jax
import jax.numpy as jnp
from jax import lax
from jax.experimental import pallas as pl
from jax.experimental.pallas import tpu as pltpu
from jax.sharding import PartitionSpec as P

DH = 128
TILE = 128
SEL = 4
RING = 4
HEADS_HERE = 5
BLOCKS = 8
TOK = BLOCKS * TILE
HALF = TOK // 2
WIDTH = HEADS_HERE * DH
FEAT = 1280
NEG = -1e30
TO_LOG2 = math.log2(math.e) / math.sqrt(DH)


def all_waited(copies):
    for copy in copies:
        copy.wait_send()


def kernel(
    ids, cnt, q_in, k_in, v_in, w_in, out,
    QB, CB, VIN, OB, OWN, RLY, OIN, LB, LRLY, LIN, AT, W, ACC,
    send_sem, recv_sem, local_sem, *kv_bufs,
):
    KB, VB = kv_bufs[:HEADS_HERE], kv_bufs[HEADS_HERE:]
    f = lax.axis_index("frames")
    py = lax.axis_index("heads")
    px = f // 8
    pz = (f // 2) % 4
    c = f % 2

    def frame(x, z, core):
        return (x * 4 + z) * 2 + core

    def up(p):
        return (p + 1) % 4

    def down(p):
        return (p + 3) % 4

    x_right, x_left = (frame(up(px), pz, c), py), (frame(down(px), pz, c), py)
    z_right, z_left = (frame(px, up(pz), c), py), (frame(px, down(pz), c), py)
    z_far = (frame(px, (pz + 2) % 4, c), py)
    x_far = (frame((px + 2) % 4, pz, c), py)
    y_right, y_left, y_far = (f, up(py)), (f, down(py)), (f, (py + 2) % 4)
    sibling = (frame(px, pz, 1 - c), py)
    partners = [x_right, x_left, z_right, z_left, x_far, z_far, y_right, y_left, y_far, sibling]

    barrier = pltpu.get_barrier_semaphore()
    for device in partners:
        pl.semaphore_signal(barrier, inc=1, device_id=device, device_id_type=MESH)
    pl.semaphore_wait(barrier, len(partners))

    used = [0]
    used_local = [0]
    sent = []

    def remote(src, dst, device):
        i = used[0]
        used[0] += 1
        return pltpu.make_async_remote_copy(
            src_ref=src, dst_ref=dst, send_sem=send_sem.at[i], recv_sem=recv_sem.at[i],
            device_id=device, device_id_type=MESH,
        )

    def local(src, dst):
        i = used_local[0]
        used_local[0] += 1
        return pltpu.make_async_copy(src, dst, local_sem.at[i])

    def go(copies):
        for copy in copies:
            copy.start()
            sent.append(copy)

    def cols(h):
        return pl.ds(h * DH, DH)

    heads = range(HEADS_HERE)
    lo, hi = pl.ds(0, HALF), pl.ds(HALF, HALF)

    def slot(s, part=None):
        if part is None:
            return pl.ds(s * BLOCKS, BLOCKS)
        return pl.ds(s * BLOCKS + part * (BLOCKS // 2), BLOCKS // 2)

    on_x, on_z = (x_right, x_left), (z_right, z_left)
    kv_way = [on_x if h % 2 == 0 else on_z for h in heads]
    q_way = [on_z if h % 2 == 0 else on_x for h in heads]

    kv = []
    for h in heads:
        kv_right, kv_left = kv_way[h]
        hc = cols(h)
        first, fwd, sib_own, sib_near, sib_far, own = [], [], [], [], [], []
        for mine, buf in ((k_in.at[:, :, hc], KB[h]), (VB[h].at[slot(0)], VB[h])):
            first.append((remote(mine, buf.at[slot(2)], kv_right),
                          remote(mine, buf.at[slot(6)], kv_left)))
            fwd.append((remote(buf.at[slot(2, 0)], buf.at[slot(4, 0)], kv_right),
                        remote(buf.at[slot(6, 1)], buf.at[slot(4, 1)], kv_left)))
            sib_own.append(remote(mine, buf.at[slot(1)], sibling))
            sib_near.append((remote(buf.at[slot(2)], buf.at[slot(3)], sibling),
                             remote(buf.at[slot(6)], buf.at[slot(7)], sibling)))
            sib_far.append((remote(buf.at[slot(4, 0)], buf.at[slot(5, 0)], sibling),
                            remote(buf.at[slot(4, 1)], buf.at[slot(5, 1)], sibling)))
        own.append(local(k_in.at[:, :, hc], KB[h].at[slot(0)]))
        kv.append((first, fwd, sib_own, sib_near, sib_far, own))

    def ring(src, buf, h, device_right, device_left):
        first = (remote(src, buf.at[1, h], device_right), remote(src, buf.at[3, h], device_left))
        fwd = (remote(buf.at[1, h, lo], buf.at[2, h, lo], device_right),
               remote(buf.at[3, h, hi], buf.at[2, h, hi], device_left))
        return first, fwd

    qs = []
    for h in heads:
        mine = q_in.at[:, cols(h)]
        first, fwd = ring(mine, QB, h, *q_way[h])
        qs.append((first, fwd, local(mine, QB.at[0, h])))
    ys = []
    for h in heads:
        near = [(remote(AT.at[0, h, lo], AT.at[1, h, lo], y_right),
                 remote(AT.at[0, h, hi], AT.at[1, h, hi], y_right)),
                (remote(AT.at[0, h, hi], AT.at[3, h, hi], y_left),
                 remote(AT.at[0, h, lo], AT.at[3, h, lo], y_left))]
        fwd = (remote(AT.at[1, h, lo], AT.at[2, h, lo], y_right),
               remote(AT.at[3, h, hi], AT.at[2, h, hi], y_left))
        ys.append((near, fwd))

    os = []
    for h in heads:
        first4, last4 = pl.ds(0, BLOCKS // 2), pl.ds(BLOCKS // 2, BLOCKS // 2)
        q_right, q_left = q_way[h]
        relay = (remote(OB.at[2, h, first4], RLY.at[0, h], q_right),
                 remote(LB.at[2, h, first4], LRLY.at[0, h], q_right),
                 remote(OB.at[2, h, last4], RLY.at[1, h], q_left),
                 remote(LB.at[2, h, last4], LRLY.at[1, h], q_left))
        back = []
        for right_half, left_half in ((last4, first4), (first4, last4)):
            back.append((
                remote(OB.at[3, h, right_half], OIN.at[0, h, right_half], q_right),
                remote(LB.at[3, h, right_half], LIN.at[0, h, right_half], q_right),
                remote(OB.at[1, h, left_half], OIN.at[1, h, left_half], q_left),
                remote(LB.at[1, h, left_half], LIN.at[1, h, left_half], q_left)))
        os.append((relay, back[0], back[1]))

    rows_w = pl.ds(pl.multiple_of(c * (WIDTH // 2), WIDTH // 2), WIDTH // 2)

    def w_cols(y):
        return pl.ds(pl.multiple_of(y * FEAT, FEAT), FEAT)

    w_first = [remote(w_in.at[rows_w, w_cols(dev[1])], W.at[s, rows_w, :], dev)
               for s, dev in ((1, y_right), (3, y_left), (2, y_far))]
    w_sib = [remote(W.at[s, rows_w, :], W.at[s, rows_w, :], sibling) for s in (1, 3, 2)]
    w_own = local(w_in.at[:, w_cols(py)], W.at[0])
    cnt_copies = [remote(CB.at[0, 0], CB.at[a, s], dev)
                  for a, devs in ((0, (z_right, z_far, z_left)), (1, (x_right, x_far, x_left)))
                  for s, dev in zip((1, 2, 3), devs)]

    def flip_values(h):
        def one(j, carry):
            VB[h][j] = VIN[j, :, cols(h)].T
            return carry
        lax.fori_loop(0, BLOCKS, one, 0)

    def issue_kv(h):
        first, _, sib_own, _, _, own = kv[h]
        go(first[0])
        go([sib_own[0]])
        for copy in own:
            copy.start()
        flip_values(h)
        go(first[1])
        go([sib_own[1]])

    def issue_q(h):
        go(qs[h][0])
        qs[h][2].start()

    def forward_kv(h):
        first, fwd, _, sib_near, _, _ = kv[h]
        for t in range(2):
            for side in range(2):
                first[t][side].wait_recv()
                go([fwd[t][side], sib_near[t][side]])

    def forward_q(h):
        for side in range(2):
            qs[h][0][side].wait_recv()
            go([qs[h][1][side]])

    def share(h):
        _, fwd, _, _, sib_far, _ = kv[h]
        for t in range(2):
            for side in range(2):
                fwd[t][side].wait_recv()
                go([sib_far[t][side]])

    def ready(h):
        _, _, sib_own, sib_near, sib_far, own = kv[h]
        for side in range(2):
            qs[h][1][side].wait_recv()
        for copy in own + [qs[h][2]]:
            copy.wait()
        for t in range(2):
            sib_own[t].wait_recv()
            for side in range(2):
                sib_near[t][side].wait_recv()
                sib_far[t][side].wait_recv()

    def attend(r, h, j):
        q = QB[r, h, block_rows(j)]
        if h % 2 == 0:
            q_block = frame(px, (pz + 4 - r) % 4, c) * BLOCKS + j
            limit = CB[0, r, pl.ds(j, 1), :]
        else:
            q_block = frame((px + 4 - r) % 4, pz, c) * BLOCKS + j
            limit = CB[1 if r else 0, r, pl.ds(j, 1), :]
        places, biases = [], []
        for s in range(SEL):
            block = ids[s, q_block]
            xs, zs, cs = block >> 6, (block >> 4) & 3, (block >> 3) & 1
            step = (px + 4 - xs) & 3 if h % 2 == 0 else (pz + 4 - zs) & 3
            places.append((step * 2 + ((cs + c) & 1)) * BLOCKS + (block & 7))
            here = jnp.where(zs == pz if h % 2 == 0 else xs == px, 0.0, NEG)
            biases.append(jnp.where(limit > s, here, NEG))
        if r == 0:
            places.append(j)
            biases.append(jnp.zeros((1, TILE), jnp.float32))
        vals = [VB[h][p] for p in places]
        scores = lax.dot_general(jnp.concatenate([KB[h][p] for p in places], axis=0), q,
                                 (((1,), (1,)), ((), ())), preferred_element_type=jnp.float32)
        scores = [scores[i * TILE : (i + 1) * TILE] for i in range(len(places))]
        top = jnp.full((1, TILE), NEG * 0.1, jnp.float32)
        for t, b in zip(scores, biases):
            top = jnp.maximum(top, jnp.max(t, axis=0, keepdims=True) * TO_LOG2 + b)
        probs = [jnp.exp2(t * TO_LOG2 + (b - top)) for t, b in zip(scores, biases)]
        total = probs[0]
        for p in probs[1:]:
            total = total + p
        total = jnp.maximum(jnp.sum(total, axis=0, keepdims=True), 1e-30)
        o = jnp.dot(jnp.concatenate(vals, axis=1),
                    jnp.concatenate([p.astype(jnp.bfloat16) for p in probs], axis=0),
                    preferred_element_type=jnp.float32)
        return o * (1.0 / total), top + jnp.log2(total)

    def merge(parts):
        top = parts[0][1]
        for _, l in parts[1:]:
            top = jnp.maximum(top, l)
        ws = [jnp.exp2(l - top) for _, l in parts]
        mass = ws[0]
        for a in ws[1:]:
            mass = mass + a
        inv = 1.0 / mass
        o = 0.0
        for (po, _), a in zip(parts, ws):
            o = o + po.astype(jnp.float32) * (a * inv)
        return o, top + jnp.log2(mass)

    def over(first_block, n, body, unroll=4):
        def some(i, carry):
            stores = [body(first_block + i * unroll + u) for u in range(unroll)]
            for store in stores:
                store()
            return carry
        if n == unroll:
            some(0, 0)
        else:
            lax.fori_loop(0, n // unroll, some, 0)

    def block_rows(j):
        return pl.ds(pl.multiple_of(j * TILE, TILE), TILE)

    def put(r, h, j, o, l):
        def store():
            OB[r, h, j] = o.astype(jnp.bfloat16)
            LB[r, h, j] = l
        return store

    def plain(r, h):
        return lambda j: put(r, h, j, *attend(r, h, j))

    def merged(r, h, side, first_block):
        return lambda j: put(r, h, j, *merge([
            attend(r, h, j),
            (RLY[side, h, j - first_block], LRLY[side, h, j - first_block])]))

    def own_part(h):
        def body(j):
            o, l = attend(0, h, j)

            def store():
                OWN[h, j] = o
                LB[0, h, j] = l
            return store
        return body

    def final(h):
        def body(j):
            parts = [(OWN[h, j], LB[0, h, j])]
            for side in range(2):
                parts.append((OIN[side, h, j], LIN[side, h, j]))
            o, _ = merge(parts)

            def store():
                AT[0, h, block_rows(j)] = o.T.astype(jnp.bfloat16)
            return store
        return body

    def y_forward(h):
        near, fwd = ys[h]
        for side in range(2):
            near[side][0].wait_recv()
            go([fwd[side]])

    def project(h):
        near, fwd = ys[h]
        for side in range(2):
            near[side][1].wait_recv()
            fwd[side].wait_recv()
        last = h == HEADS_HERE - 1
        tile_n, tile_m = 256, 256

        def one(i, carry):
            cs = pl.ds(pl.multiple_of(i * tile_n, tile_n), tile_n)
            rhs = jnp.concatenate([W[r, pl.ds(h * DH, DH), cs] for r in range(RING)], axis=0)
            for m in range(TOK // tile_m):
                rs = pl.ds(m * tile_m, tile_m)
                lhs = jnp.concatenate([AT[r, h, rs] for r in range(RING)], axis=1)
                term = jnp.dot(lhs, rhs, preferred_element_type=jnp.float32)
                if h > 0:
                    term = term + ACC[rs, cs]
                if last:
                    out[rs, cs] = term.astype(jnp.bfloat16)
                else:
                    ACC[rs, cs] = term
            return carry

        lax.fori_loop(0, FEAT // tile_n, one, 0)

    values_in = local(v_in, VIN)
    values_in.start()
    for j in range(BLOCKS):
        CB[0, 0, pl.ds(j, 1), :] = jnp.full((1, 128), cnt[j], jnp.int32)
    values_in.wait()

    def far_part(h):
        over(0, 8, plain(2, h))
        go(os[h][0])

    def near_part(h):
        over(4, 4, plain(3, h))
        over(0, 4, plain(1, h))
        go(os[h][1])
        over(0, 8, own_part(h))

    def merge_part(h):
        for copy in os[h][0]:
            copy.wait_recv()
        over(0, 4, merged(3, h, 0, 0))
        over(4, 4, merged(1, h, 1, 4))
        go(os[h][2])

    def finish(h):
        for copy in os[h][1] + os[h][2]:
            copy.wait_recv()
        (right_lo, right_hi), (left_hi, left_lo) = ys[h][0]
        over(0, 4, final(h))
        go([right_lo])
        over(4, 4, final(h))
        go([left_hi, right_hi, left_lo])

    def weights(step):
        if step == 0:
            go(cnt_copies)
            go(w_first)
            w_own.start()
        elif step == 1:
            for copy in cnt_copies:
                copy.wait_recv()
        elif step == 2:
            for a, b in zip(w_first, w_sib):
                a.wait_recv()
                go([b])
        else:
            for copy in w_sib:
                copy.wait_recv()
            w_own.wait()

    issue_q(1)
    issue_q(2)
    issue_q(0)
    issue_kv(3)
    weights(0)
    issue_kv(0)
    issue_kv(2)
    forward_kv(0)
    issue_kv(1)
    forward_q(1)
    forward_kv(2)
    forward_q(0)
    forward_kv(1)
    issue_kv(4)
    share(0)
    forward_kv(3)
    ready(0)
    weights(1)
    far_part(0)
    share(1)
    forward_q(2)
    near_part(0)
    ready(1)
    share(2)
    far_part(1)
    near_part(1)
    issue_q(3)
    share(3)
    merge_part(0)
    ready(2)
    near_part(2)
    far_part(2)
    finish(0)
    merge_part(1)
    issue_q(4)
    y_forward(0)
    forward_q(3)
    forward_kv(4)
    merge_part(2)
    finish(1)
    ready(3)
    forward_q(4)
    weights(2)
    far_part(3)
    finish(2)
    near_part(3)
    share(4)
    weights(3)
    y_forward(1)
    merge_part(3)
    y_forward(2)
    ready(4)
    far_part(4)
    near_part(4)
    finish(3)
    merge_part(4)
    project(0)
    y_forward(3)
    project(1)
    finish(4)
    project(2)
    project(3)
    y_forward(4)
    project(4)

    all_waited(sent)


MESH = pl.DeviceIdType.MESH
N_REMOTE = 5 * (18 + 4 + 4 + 8) + 6 + 6
N_REMOTE = 5 * (18 + 4 + 12 + 6) + 6 + 6
N_LOCAL = 5 * 2 + 2


def shards(queries, keys, values, block_ids, counts, w_out):
    smem = pl.BlockSpec(memory_space=pltpu.SMEM)
    vmem = pl.BlockSpec(memory_space=pltpu.VMEM)
    hbm = pl.BlockSpec(memory_space=pl.ANY)
    bf16, f32 = jnp.bfloat16, jnp.float32
    return pl.pallas_call(
        kernel,
        out_shape=jax.ShapeDtypeStruct((TOK, FEAT), bf16),
        in_specs=[smem, smem, hbm, hbm, hbm, hbm],
        out_specs=vmem,
        scratch_shapes=[
            pltpu.VMEM((4, HEADS_HERE, TOK, DH), bf16),
            pltpu.VMEM((2, 4, BLOCKS, 128), jnp.int32),
            pltpu.VMEM((BLOCKS, TILE, WIDTH), bf16),
            pltpu.VMEM((4, HEADS_HERE, BLOCKS, DH, TILE), bf16),
            pltpu.VMEM((HEADS_HERE, BLOCKS, DH, TILE), f32),
            pltpu.VMEM((2, HEADS_HERE, BLOCKS // 2, DH, TILE), bf16),
            pltpu.VMEM((2, HEADS_HERE, BLOCKS, DH, TILE), bf16),
            pltpu.VMEM((4, HEADS_HERE, BLOCKS, 1, 128), f32),
            pltpu.VMEM((2, HEADS_HERE, BLOCKS // 2, 1, 128), f32),
            pltpu.VMEM((2, HEADS_HERE, BLOCKS, 1, 128), f32),
            pltpu.VMEM((4, HEADS_HERE, TOK, DH), bf16),
            pltpu.VMEM((4, WIDTH, FEAT), bf16),
            pltpu.VMEM((TOK, FEAT), f32),
            pltpu.SemaphoreType.DMA((N_REMOTE,)),
            pltpu.SemaphoreType.DMA((N_REMOTE,)),
            pltpu.SemaphoreType.DMA((N_LOCAL,)),
        ] + [pltpu.VMEM((8 * BLOCKS, TILE, DH), bf16)] * (2 * HEADS_HERE),
        compiler_params=pltpu.CompilerParams(
            collective_id=0, has_side_effects=True, vmem_limit_bytes=67043328),
        name="sparse_attention",
    )(block_ids.T, counts, queries, keys.reshape(BLOCKS, TILE, WIDTH), values.reshape(BLOCKS, TILE, WIDTH), w_out)


def solution(mesh):
    placed = (
        P("frames", "heads"),
        P("frames", "heads"),
        P("frames", "heads"),
        P(),
        P("frames"),
        P("heads", None),
    )
    return jax.shard_map(
        shards, mesh=mesh, in_specs=placed, out_specs=P("frames", "heads"), check_vma=False
    )
```

```python
import math

import jax
import jax.numpy as jnp
from jax import lax
from jax.experimental import pallas as pl
from jax.experimental.pallas import tpu as pltpu
from jax.sharding import PartitionSpec as P

DH = 128
TILE = 128
SEL = 4
RING = 4
HEADS_HERE = 5
BLOCKS = 8
TOK = BLOCKS * TILE
HALF = TOK // 2
WIDTH = HEADS_HERE * DH
FEAT = 1280
NEG = -1e30
TO_LOG2 = math.log2(math.e) / math.sqrt(DH)


def all_waited(copies):
    for copy in copies:
        copy.wait_send()


def kernel(
    ids, cnt, q_in, k_in, v_in, w_in, out,
    QB, CB, VIN, OB, OWN, RLY, OIN, LB, LRLY, LIN, AT, W, ACC,
    send_sem, recv_sem, local_sem, *kv_bufs,
):
    KB, VB = kv_bufs[:HEADS_HERE], kv_bufs[HEADS_HERE:]
    f = lax.axis_index("frames")
    py = lax.axis_index("heads")
    px = f // 8
    pz = (f // 2) % 4
    c = f % 2

    def frame(x, z, core):
        return (x * 4 + z) * 2 + core

    def up(p):
        return (p + 1) % 4

    def down(p):
        return (p + 3) % 4

    x_right, x_left = (frame(up(px), pz, c), py), (frame(down(px), pz, c), py)
    z_right, z_left = (frame(px, up(pz), c), py), (frame(px, down(pz), c), py)
    z_far = (frame(px, (pz + 2) % 4, c), py)
    x_far = (frame((px + 2) % 4, pz, c), py)
    y_right, y_left, y_far = (f, up(py)), (f, down(py)), (f, (py + 2) % 4)
    sibling = (frame(px, pz, 1 - c), py)
    partners = [x_right, x_left, z_right, z_left, x_far, z_far, y_right, y_left, y_far, sibling]

    values_in = pltpu.make_async_copy(v_in, VIN, local_sem.at[N_LOCAL - 1])
    values_in.start()
    for j in range(BLOCKS):
        CB[0, 0, pl.ds(j, 1), :] = jnp.full((1, 128), cnt[j], jnp.int32)

    barrier = pltpu.get_barrier_semaphore()
    for device in partners:
        pl.semaphore_signal(barrier, inc=1, device_id=device, device_id_type=MESH)
    pl.semaphore_wait(barrier, len(partners))

    used = [0]
    used_local = [0]
    sent = []

    def remote(src, dst, device):
        i = used[0]
        used[0] += 1
        return pltpu.make_async_remote_copy(
            src_ref=src, dst_ref=dst, send_sem=send_sem.at[i], recv_sem=recv_sem.at[i],
            device_id=device, device_id_type=MESH,
        )

    def local(src, dst):
        i = used_local[0]
        used_local[0] += 1
        return pltpu.make_async_copy(src, dst, local_sem.at[i])

    def go(copies):
        for copy in copies:
            copy.start()
            sent.append(copy)

    def cols(h):
        return pl.ds(h * DH, DH)

    heads = range(HEADS_HERE)
    lo, hi = pl.ds(0, HALF), pl.ds(HALF, HALF)

    def slot(s, part=None):
        if part is None:
            return pl.ds(s * BLOCKS, BLOCKS)
        return pl.ds(s * BLOCKS + part * (BLOCKS // 2), BLOCKS // 2)

    on_x, on_z = (x_right, x_left), (z_right, z_left)
    kv_way = [on_x if h % 2 == 0 else on_z for h in heads]
    q_way = [on_z if h % 2 == 0 else on_x for h in heads]

    kv = []
    for h in heads:
        kv_right, kv_left = kv_way[h]
        hc = cols(h)
        first, fwd, sib_own, sib_near, sib_far, own = [], [], [], [], [], []
        for mine, buf in ((k_in.at[:, :, hc], KB[h]), (VB[h].at[slot(0)], VB[h])):
            first.append((remote(mine, buf.at[slot(2)], kv_right),
                          remote(mine, buf.at[slot(6)], kv_left)))
            fwd.append((remote(buf.at[slot(2, 0)], buf.at[slot(4, 0)], kv_right),
                        remote(buf.at[slot(6, 1)], buf.at[slot(4, 1)], kv_left)))
            sib_own.append(remote(mine, buf.at[slot(1)], sibling))
            sib_near.append((remote(buf.at[slot(2)], buf.at[slot(3)], sibling),
                             remote(buf.at[slot(6)], buf.at[slot(7)], sibling)))
            sib_far.append((remote(buf.at[slot(4, 0)], buf.at[slot(5, 0)], sibling),
                            remote(buf.at[slot(4, 1)], buf.at[slot(5, 1)], sibling)))
        own.append(local(k_in.at[:, :, hc], KB[h].at[slot(0)]))
        kv.append((first, fwd, sib_own, sib_near, sib_far, own))

    def ring(src, buf, h, device_right, device_left):
        first = (remote(src, buf.at[1, h], device_right), remote(src, buf.at[3, h], device_left))
        fwd = (remote(buf.at[1, h, lo], buf.at[2, h, lo], device_right),
               remote(buf.at[3, h, hi], buf.at[2, h, hi], device_left))
        return first, fwd

    qs = []
    for h in heads:
        mine = q_in.at[:, cols(h)]
        first, fwd = ring(mine, QB, h, *q_way[h])
        qs.append((first, fwd, local(mine, QB.at[0, h])))
    ys = []
    for h in heads:
        near = [(remote(AT.at[0, h, lo], AT.at[1, h, lo], y_right),
                 remote(AT.at[0, h, hi], AT.at[1, h, hi], y_right)),
                (remote(AT.at[0, h, hi], AT.at[3, h, hi], y_left),
                 remote(AT.at[0, h, lo], AT.at[3, h, lo], y_left))]
        fwd = (remote(AT.at[1, h, lo], AT.at[2, h, lo], y_right),
               remote(AT.at[3, h, hi], AT.at[2, h, hi], y_left))
        ys.append((near, fwd))

    def pieces(h):
        return 2 if h == HEADS_HERE - 1 else 1

    def span(h):
        return BLOCKS // 2 // pieces(h)

    def piece(h, side, p):
        return pl.ds(side * (BLOCKS // 2) + p * span(h), span(h))

    os = []
    for h in heads:
        q_right, q_left = q_way[h]
        relays, middles = [], []
        for p in range(pieces(h)):
            near, far = piece(h, 0, p), piece(h, 1, p)
            place = pl.ds(p * span(h), span(h))
            relays.append((
                (remote(OB.at[2, h, near], RLY.at[0, h, place], q_right),
                 remote(LB.at[2, h, near], LRLY.at[0, h, place], q_right)),
                (remote(OB.at[2, h, far], RLY.at[1, h, place], q_left),
                 remote(LB.at[2, h, far], LRLY.at[1, h, place], q_left))))
            middles.append((
                (remote(OB.at[3, h, near], OIN.at[0, h, near], q_right),
                 remote(LB.at[3, h, near], LIN.at[0, h, near], q_right)),
                (remote(OB.at[1, h, far], OIN.at[1, h, far], q_left),
                 remote(LB.at[1, h, far], LIN.at[1, h, far], q_left))))
        first4, last4 = pl.ds(0, BLOCKS // 2), pl.ds(BLOCKS // 2, BLOCKS // 2)
        ends = (remote(OB.at[3, h, last4], OIN.at[0, h, last4], q_right),
                remote(LB.at[3, h, last4], LIN.at[0, h, last4], q_right),
                remote(OB.at[1, h, first4], OIN.at[1, h, first4], q_left),
                remote(LB.at[1, h, first4], LIN.at[1, h, first4], q_left))
        os.append((relays, ends, middles))

    rows_w = pl.ds(pl.multiple_of(c * (WIDTH // 2), WIDTH // 2), WIDTH // 2)

    def w_cols(y):
        return pl.ds(pl.multiple_of(y * FEAT, FEAT), FEAT)

    w_first = [remote(w_in.at[rows_w, w_cols(dev[1])], W.at[s, rows_w, :], dev)
               for s, dev in ((1, y_right), (3, y_left), (2, y_far))]
    w_sib = [remote(W.at[s, rows_w, :], W.at[s, rows_w, :], sibling) for s in (1, 3, 2)]
    w_own = local(w_in.at[:, w_cols(py)], W.at[0])
    cnt_copies = [remote(CB.at[0, 0], CB.at[a, s], dev)
                  for a, devs in ((0, (z_right, z_far, z_left)), (1, (x_right, x_far, x_left)))
                  for s, dev in zip((1, 2, 3), devs)]

    def flip_values(h):
        def one(j, carry):
            VB[h][j] = VIN[j, :, cols(h)].T
            return carry
        lax.fori_loop(0, BLOCKS, one, 0)

    values_waited = []

    def issue_kv(h):
        first, _, sib_own, _, _, own = kv[h]
        go(first[0])
        go([sib_own[0]])
        for copy in own:
            copy.start()
        if not values_waited:
            values_waited.append(True)
            values_in.wait()
        flip_values(h)
        go(first[1])
        go([sib_own[1]])

    def issue_q(h):
        go(qs[h][0])
        qs[h][2].start()

    def forward_kv(h):
        first, fwd, _, sib_near, _, _ = kv[h]
        for t in range(2):
            for side in range(2):
                first[t][side].wait_recv()
                go([fwd[t][side], sib_near[t][side]])

    def forward_q(h):
        for side in range(2):
            qs[h][0][side].wait_recv()
            go([qs[h][1][side]])

    def share(h):
        _, fwd, _, _, sib_far, _ = kv[h]
        for t in range(2):
            for side in range(2):
                fwd[t][side].wait_recv()
                go([sib_far[t][side]])

    def ready(h):
        _, _, sib_own, sib_near, sib_far, own = kv[h]
        for side in range(2):
            qs[h][1][side].wait_recv()
        for copy in own + [qs[h][2]]:
            copy.wait()
        for t in range(2):
            sib_own[t].wait_recv()
            for side in range(2):
                sib_near[t][side].wait_recv()
                sib_far[t][side].wait_recv()

    def attend(r, h, j):
        q = QB[r, h, block_rows(j)]
        if h % 2 == 0:
            q_block = frame(px, (pz + 4 - r) % 4, c) * BLOCKS + j
            limit = CB[0, r, pl.ds(j, 1), :]
        else:
            q_block = frame((px + 4 - r) % 4, pz, c) * BLOCKS + j
            limit = CB[1 if r else 0, r, pl.ds(j, 1), :]
        places, biases = [], []
        for s in range(SEL):
            block = ids[s, q_block]
            xs, zs, cs = block >> 6, (block >> 4) & 3, (block >> 3) & 1
            step = (px + 4 - xs) & 3 if h % 2 == 0 else (pz + 4 - zs) & 3
            places.append((step * 2 + ((cs + c) & 1)) * BLOCKS + (block & 7))
            here = jnp.where(zs == pz if h % 2 == 0 else xs == px, 0.0, NEG)
            biases.append(jnp.where(limit > s, here, NEG))
        if r == 0:
            places.append(j)
            biases.append(jnp.zeros((1, TILE), jnp.float32))
        vals = [VB[h][p] for p in places]
        scores = lax.dot_general(jnp.concatenate([KB[h][p] for p in places], axis=0), q,
                                 (((1,), (1,)), ((), ())), preferred_element_type=jnp.float32)
        scores = [scores[i * TILE : (i + 1) * TILE] for i in range(len(places))]
        top = jnp.full((1, TILE), NEG * 0.1, jnp.float32)
        for t, b in zip(scores, biases):
            top = jnp.maximum(top, jnp.max(t, axis=0, keepdims=True) * TO_LOG2 + b)
        probs = [jnp.exp2(t * TO_LOG2 + (b - top)) for t, b in zip(scores, biases)]
        total = probs[0]
        for p in probs[1:]:
            total = total + p
        total = jnp.maximum(jnp.sum(total, axis=0, keepdims=True), 1e-30)
        o = jnp.dot(jnp.concatenate(vals, axis=1),
                    jnp.concatenate([p.astype(jnp.bfloat16) for p in probs], axis=0),
                    preferred_element_type=jnp.float32)
        return o * (1.0 / total), top + jnp.log2(total)

    def merge(parts):
        top = parts[0][1]
        for _, l in parts[1:]:
            top = jnp.maximum(top, l)
        ws = [jnp.exp2(l - top) for _, l in parts]
        mass = ws[0]
        for a in ws[1:]:
            mass = mass + a
        inv = 1.0 / mass
        o = 0.0
        for (po, _), a in zip(parts, ws):
            o = o + po.astype(jnp.float32) * (a * inv)
        return o, top + jnp.log2(mass)

    def over(first_block, n, body, unroll=4):
        def some(i, carry):
            stores = [body(first_block + i * unroll + u) for u in range(unroll)]
            for store in stores:
                store()
            return carry
        if n == unroll:
            some(0, 0)
        else:
            lax.fori_loop(0, n // unroll, some, 0)

    def block_rows(j):
        return pl.ds(pl.multiple_of(j * TILE, TILE), TILE)

    def put(r, h, j, o, l):
        def store():
            OB[r, h, j] = o.astype(jnp.bfloat16)
            LB[r, h, j] = l
        return store

    def plain(r, h):
        return lambda j: put(r, h, j, *attend(r, h, j))

    def merged(r, h, side, first_block):
        return lambda j: put(r, h, j, *merge([
            attend(r, h, j),
            (RLY[side, h, j - first_block], LRLY[side, h, j - first_block])]))

    def own_part(h):
        def body(j):
            o, l = attend(0, h, j)

            def store():
                OWN[h, j] = o
                LB[0, h, j] = l
            return store
        return body

    def final(h):
        def body(j):
            parts = [(OWN[h, j], LB[0, h, j])]
            for side in range(2):
                parts.append((OIN[side, h, j], LIN[side, h, j]))
            o, _ = merge(parts)

            def store():
                AT[0, h, block_rows(j)] = o.T.astype(jnp.bfloat16)
            return store
        return body

    def y_forward(h):
        near, fwd = ys[h]
        for side in range(2):
            near[side][0].wait_recv()
            go([fwd[side]])

    def project(h):
        near, fwd = ys[h]
        for side in range(2):
            near[side][1].wait_recv()
            fwd[side].wait_recv()
        last = h == HEADS_HERE - 1
        tile_n, tile_m = 256, 256

        def one(i, carry):
            cs = pl.ds(pl.multiple_of(i * tile_n, tile_n), tile_n)
            rhs = jnp.concatenate([W[r, pl.ds(h * DH, DH), cs] for r in range(RING)], axis=0)
            for m in range(TOK // tile_m):
                rs = pl.ds(m * tile_m, tile_m)
                lhs = jnp.concatenate([AT[r, h, rs] for r in range(RING)], axis=1)
                term = jnp.dot(lhs, rhs, preferred_element_type=jnp.float32)
                if h > 0:
                    term = term + ACC[rs, cs]
                if last:
                    out[rs, cs] = term.astype(jnp.bfloat16)
                else:
                    ACC[rs, cs] = term
            return carry

        lax.fori_loop(0, FEAT // tile_n, one, 0)

    def far_part(h):
        relays = os[h][0]
        over(0, 4, plain(2, h))
        for relay in relays:
            go(relay[0])
        over(4, 4, plain(2, h))
        for relay in relays:
            go(relay[1])

    def near_part(h):
        over(4, 4, plain(3, h))
        over(0, 4, plain(1, h))
        go(os[h][1])
        over(0, 8, own_part(h))

    def merge_part(h):
        relays, _, middles = os[h]
        n = span(h)
        for relay, middle, p in zip(relays, middles, range(pieces(h))):
            for side, r in ((0, 3), (1, 1)):
                for copy in relay[side]:
                    copy.wait_recv()
                over(side * 4 + p * n, n, merged(r, h, side, side * 4), n)
                go(middle[side])

    def finish(h):
        _, ends, middles = os[h]
        (right_lo, right_hi), (left_hi, left_lo) = ys[h][0]
        n = span(h)
        for copy in ends:
            copy.wait_recv()
        for side in range(2):
            for p, middle in enumerate(middles):
                for copy in middle[side]:
                    copy.wait_recv()
                over(side * 4 + p * n, n, final(h), n)
            if side == 0:
                go([right_lo])
        go([left_hi, right_hi, left_lo])

    def weights(step):
        if step == 0:
            go(cnt_copies)
            go(w_first)
            w_own.start()
        elif step == 1:
            for copy in cnt_copies:
                copy.wait_recv()
        elif step == 2:
            for a, b in zip(w_first, w_sib):
                a.wait_recv()
                go([b])
        else:
            for copy in w_sib:
                copy.wait_recv()
            w_own.wait()

    issue_q(0)
    issue_kv(2)
    issue_q(2)
    issue_q(1)
    issue_q(3)
    issue_kv(1)
    forward_kv(2)
    weights(0)
    issue_kv(0)
    forward_kv(1)
    forward_q(2)
    issue_kv(3)
    weights(1)
    forward_q(0)
    share(1)
    forward_q(1)
    share(2)
    ready(2)
    far_part(2)
    forward_kv(0)
    forward_kv(3)
    ready(1)
    far_part(1)
    issue_kv(4)
    share(0)
    near_part(2)
    merge_part(2)
    share(3)
    ready(0)
    far_part(0)
    issue_q(4)
    near_part(1)
    finish(2)
    merge_part(1)
    forward_q(3)
    merge_part(0)
    weights(2)
    forward_kv(4)
    y_forward(2)
    near_part(0)
    finish(1)
    ready(3)
    far_part(3)
    finish(0)
    y_forward(1)
    forward_q(4)
    near_part(3)
    share(4)
    weights(3)
    merge_part(3)
    ready(4)
    far_part(4)
    y_forward(0)
    near_part(4)
    finish(3)
    merge_part(4)
    y_forward(3)
    finish(4)
    project(0)
    project(1)
    project(2)
    y_forward(4)
    project(3)
    project(4)

    all_waited(sent)


MESH = pl.DeviceIdType.MESH
N_REMOTE = 5 * (18 + 4 + 4 + 8) + 6 + 6
N_REMOTE = 5 * (18 + 4 + 12 + 6) + 8 + 6 + 6
N_LOCAL = 5 * 2 + 2


def shards(queries, keys, values, block_ids, counts, w_out):
    smem = pl.BlockSpec(memory_space=pltpu.SMEM)
    vmem = pl.BlockSpec(memory_space=pltpu.VMEM)
    hbm = pl.BlockSpec(memory_space=pl.ANY)
    bf16, f32 = jnp.bfloat16, jnp.float32
    return pl.pallas_call(
        kernel,
        out_shape=jax.ShapeDtypeStruct((TOK, FEAT), bf16),
        in_specs=[smem, smem, hbm, hbm, hbm, hbm],
        out_specs=vmem,
        scratch_shapes=[
            pltpu.VMEM((4, HEADS_HERE, TOK, DH), bf16),
            pltpu.VMEM((2, 4, BLOCKS, 128), jnp.int32),
            pltpu.VMEM((BLOCKS, TILE, WIDTH), bf16),
            pltpu.VMEM((4, HEADS_HERE, BLOCKS, DH, TILE), bf16),
            pltpu.VMEM((HEADS_HERE, BLOCKS, DH, TILE), f32),
            pltpu.VMEM((2, HEADS_HERE, BLOCKS // 2, DH, TILE), bf16),
            pltpu.VMEM((2, HEADS_HERE, BLOCKS, DH, TILE), bf16),
            pltpu.VMEM((4, HEADS_HERE, BLOCKS, 1, 128), f32),
            pltpu.VMEM((2, HEADS_HERE, BLOCKS // 2, 1, 128), f32),
            pltpu.VMEM((2, HEADS_HERE, BLOCKS, 1, 128), f32),
            pltpu.VMEM((4, HEADS_HERE, TOK, DH), bf16),
            pltpu.VMEM((4, WIDTH, FEAT), bf16),
            pltpu.VMEM((TOK, FEAT), f32),
            pltpu.SemaphoreType.DMA((N_REMOTE,)),
            pltpu.SemaphoreType.DMA((N_REMOTE,)),
            pltpu.SemaphoreType.DMA((N_LOCAL,)),
        ] + [pltpu.VMEM((8 * BLOCKS, TILE, DH), bf16)] * (2 * HEADS_HERE),
        compiler_params=pltpu.CompilerParams(
            collective_id=0, has_side_effects=True, vmem_limit_bytes=67043328),
        name="sparse_attention",
    )(block_ids.T, counts, queries, keys.reshape(BLOCKS, TILE, WIDTH), values.reshape(BLOCKS, TILE, WIDTH), w_out)


def solution(mesh):
    placed = (
        P("frames", "heads"),
        P("frames", "heads"),
        P("frames", "heads"),
        P(),
        P("frames"),
        P("heads", None),
    )
    return jax.shard_map(
        shards, mesh=mesh, in_specs=placed, out_specs=P("frames", "heads"), check_vma=False
    )
```
